32 devices in a mesh: part: 1 (over z), data: 4 (over y), stage: 8 (over x, core).
Axes of the slice: x: 4, y: 4, z: 1, core: 2. Of those that a mesh axis runs over, the one named last changes fastest.
The devices are a block of a 4x4x8 slice.
Arguments:
- x_in: bfloat16 [8, 64, 512], P(('part', 'data'))
- y_tgt: bfloat16 [8, 64, 512], P(('part', 'data'))
- w_up: bfloat16 [32, 512, 2048], P('stage')
- w_down: bfloat16 [32, 2048, 512], P('stage')
- gain: float32 [32, 512], P('stage')
Outputs:
- output 1: float32 [32, 512, 2048], P(('part', 'stage'))
- output 2: float32 [32, 2048, 512], P(('part', 'stage'))
- output 3: float32 [32, 512], P(('part', 'stage'))
- output 4: float32 [1], P('part')
All inputs are finite; a program needn't handle non-finite values.
Results may differ from the reference program's by a relative error of at most 0.0155895.
Values are sent between devices in bfloat16 or wider.
A program may use at most 768 MiB of HBM per device.

```python
import jax
import jax.numpy as jnp
from jax import lax

MICRO_ALL = 8
TOKENS = 64
D = 512
FF = 2048
LAYERS = 32
EPS = 1e-6
TOK_TOTAL = MICRO_ALL * TOKENS


def setup_inputs(seed: int = 0, part: int = 0) -> dict:
    base_key = jax.random.key(seed)
    key_up, key_down, key_gain, key_data = jax.random.split(base_key, 4)
    key_x, key_y = jax.random.split(jax.random.fold_in(key_data, part), 2)
    w_up = (jax.random.normal(key_up, (LAYERS, D, FF), jnp.float32) * D ** -0.5).astype(jnp.bfloat16)
    w_down = (jax.random.normal(key_down, (LAYERS, FF, D), jnp.float32) * FF ** -0.5).astype(jnp.bfloat16)
    gain = 1.0 + 0.25 * jax.random.normal(key_gain, (LAYERS, D), jnp.float32)
    x_in = jax.random.normal(key_x, (MICRO_ALL, TOKENS, D), jnp.float32).astype(jnp.bfloat16)
    y_tgt = jax.random.normal(key_y, (MICRO_ALL, TOKENS, D), jnp.float32).astype(jnp.bfloat16)
    return {"x_in": x_in, "y_tgt": y_tgt, "w_up": w_up, "w_down": w_down, "gain": gain}


def layer_fwd(x_rows, w_one, w_two, gain_row):
    x_float = x_rows.astype(jnp.float32)
    inv_rms = lax.rsqrt(jnp.mean(x_float * x_float, axis=-1, keepdims=True) + EPS)
    normed = (x_float * inv_rms * gain_row).astype(jnp.bfloat16)
    pre_act = jnp.dot(normed, w_one, preferred_element_type=jnp.float32)
    hidden = jax.nn.gelu(pre_act).astype(jnp.bfloat16)
    update = jnp.dot(hidden, w_two, preferred_element_type=jnp.float32)
    return (x_float + update).astype(jnp.bfloat16)


def layer_bwd(x_rows, d_out, w_one, w_two, gain_row):
    x_float = x_rows.astype(jnp.float32)
    inv_rms = lax.rsqrt(jnp.mean(x_float * x_float, axis=-1, keepdims=True) + EPS)
    unit_x = x_float * inv_rms
    normed = (unit_x * gain_row).astype(jnp.bfloat16)
    pre_act = jnp.dot(normed, w_one, preferred_element_type=jnp.float32)
    act_full, gelu_back = jax.vjp(jax.nn.gelu, pre_act)
    hidden = act_full.astype(jnp.bfloat16)
    g_two = jnp.dot(hidden.T, d_out, preferred_element_type=jnp.float32)
    d_hidden = jnp.dot(d_out, w_two.T, preferred_element_type=jnp.float32)
    d_pre = gelu_back(d_hidden)[0].astype(jnp.bfloat16)
    g_one = jnp.dot(normed.T, d_pre, preferred_element_type=jnp.float32)
    d_normed = jnp.dot(d_pre, w_one.T, preferred_element_type=jnp.float32)
    g_gain = jnp.sum(d_normed * unit_x, axis=0)
    d_unit = d_normed * gain_row
    d_x = inv_rms * (d_unit - unit_x * jnp.mean(d_unit * unit_x, axis=-1, keepdims=True))
    return (d_out.astype(jnp.float32) + d_x).astype(jnp.bfloat16), g_one, g_two, g_gain


def reference(x_in, y_tgt, w_up, w_down, gain):
    def micro_step(state_in, mb_pair):
        acc_one, acc_two, acc_gain, loss_sum = state_in
        x_now, y_now = mb_pair

        def fwd_body(hidden_x, layer_w):
            w_one, w_two, gain_row = layer_w
            return layer_fwd(hidden_x, w_one, w_two, gain_row), hidden_x

        top_out, saved_x = lax.scan(fwd_body, x_now, (w_up, w_down, gain))
        err_top = top_out.astype(jnp.float32) - y_now.astype(jnp.float32)
        d_top = (err_top / TOK_TOTAL).astype(jnp.bfloat16)

        def bwd_body(d_rows, layer_item):
            x_saved, w_one, w_two, gain_row = layer_item
            d_next, g_one, g_two, g_gain = layer_bwd(x_saved, d_rows, w_one, w_two, gain_row)
            return d_next, (g_one, g_two, g_gain)

        layer_grads = lax.scan(bwd_body, d_top, (saved_x, w_up, w_down, gain), reverse=True)[1]
        new_state = (acc_one + layer_grads[0], acc_two + layer_grads[1], acc_gain + layer_grads[2], loss_sum + jnp.sum(err_top * err_top))
        return new_state, None

    init_state = (jnp.zeros((LAYERS, D, FF), jnp.float32), jnp.zeros((LAYERS, FF, D), jnp.float32), jnp.zeros((LAYERS, D), jnp.float32), jnp.zeros((), jnp.float32))
    final_state = lax.scan(micro_step, init_state, (x_in, y_tgt))[0]
    d_up, d_down, d_gain, loss_sum = final_state
    loss_out = (loss_sum / (TOK_TOTAL * D)).reshape(1)
    return d_up, d_down, d_gain, loss_out
```

```python
import functools

import jax
import jax.numpy as jnp
from jax import lax
from jax.experimental import pallas as pl
from jax.experimental.pallas import tpu as pltpu
from jax.sharding import PartitionSpec as P

EPS = 1e-6
C1 = 0.7978845608028654
C2 = C1 * 0.044715
MESH = pl.DeviceIdType.MESH
BF = jnp.bfloat16
F32 = jnp.float32


def dot(lhs, rhs):
    return jnp.dot(lhs, rhs, preferred_element_type=F32)


def gelu_tanh(pre):
    sq = pre * pre
    return sq, jnp.tanh(pre * (C1 + C2 * sq))


def gelu_val(pre, th):
    half = 0.5 * pre
    return (half + half * th).astype(BF)


def gelu_grad(pre, sq, th):
    return (0.5 + 0.5 * th) + (0.5 * pre) * (1.0 - th * th) * (C1 + (3.0 * C2) * sq)


def unit_rows(rows):
    x_float = rows.astype(F32)
    inv_rms = lax.rsqrt(jnp.mean(x_float * x_float, axis=-1, keepdims=True) + EPS)
    return x_float, inv_rms, x_float * inv_rms


def chain_kernel(
    n_data, n_stage, tok_total, fc,
    x_hbm, y_hbm, w1_hbm, w2_hbm, gain_ref,
    rt_hbm, ut_hbm, da_hbm, dh_hbm, dgain_ref, loss_ref,
    w1s, w2s, w1t, w2t, xs, dhs, gps, dao, dast, utst, rtst, ybuf, dgs, lossb, losst,
    w1_sem, w2_sem, x_sem, y_sem, xsend, xrecv, dsend, drecv, cs_send, cs_recv, cd_send, cd_recv,
    gsend, grecv, lsend, lrecv, ls_send, ls_recv, ut_sem, rt_sem, da_sem, dao_sem, dh_sem,
):
    rep = lax.axis_index("data")
    stage = lax.axis_index("stage")
    depth, width, ff = w1s.shape
    rows = xs.shape[2]
    n_chunk = ff // fc
    last = n_stage - 1
    is_late = stage >= n_stage - 2

    def peer(step):
        return lax.rem(rep + step, n_data)

    barrier = pltpu.get_barrier_semaphore()
    for step in range(1, n_data):
        pl.semaphore_signal(barrier, inc=1, device_id={"data": peer(step)}, device_id_type=MESH)
    pl.semaphore_signal(barrier, inc=1, device_id={"stage": lax.rem(stage + 1, n_stage)}, device_id_type=MESH)
    pl.semaphore_signal(barrier, inc=1, device_id={"stage": lax.rem(stage + last, n_stage)}, device_id_type=MESH)

    def w1_copy(l):
        return pltpu.make_async_copy(w1_hbm.at[l], w1s.at[l], w1_sem.at[l])

    def w2_copy(l):
        return pltpu.make_async_copy(w2_hbm.at[l], w2s.at[l], w2_sem.at[l])

    x_copy = pltpu.make_async_copy(x_hbm, xs.at[0, rep], x_sem)
    y_copy = pltpu.make_async_copy(y_hbm, ybuf, y_sem)

    @pl.when(stage == 0)
    def _():
        x_copy.start()

    for l in range(depth):
        w1_copy(l).start()
        w2_copy(l).start()

    @pl.when(stage == last)
    def _():
        y_copy.start()

    pl.semaphore_wait(barrier, n_data + 1)

    def gather_send(buf, slot, send, recv, l, step):
        return pltpu.make_async_remote_copy(
            src_ref=buf.at[slot, rep], dst_ref=buf.at[slot, rep],
            send_sem=send.at[l, step - 1], recv_sem=recv.at[l, rep],
            device_id={"data": peer(step)}, device_id_type=MESH)

    def gather_recv(buf, slot, send, recv, l, who):
        return pltpu.make_async_remote_copy(
            src_ref=buf.at[slot, who], dst_ref=buf.at[slot, who],
            send_sem=send.at[l, 0], recv_sem=recv.at[l, who],
            device_id={"data": peer(1)}, device_id_type=MESH)

    chain_fwd = pltpu.make_async_remote_copy(
        src_ref=xs.at[depth, rep], dst_ref=xs.at[0, rep], send_sem=cs_send, recv_sem=cs_recv,
        device_id={"stage": lax.rem(stage + 1, n_stage)}, device_id_type=MESH)
    chain_bwd = pltpu.make_async_remote_copy(
        src_ref=dhs.at[0, rep], dst_ref=dhs.at[depth, rep], send_sem=cd_send, recv_sem=cd_recv,
        device_id={"stage": lax.rem(stage + last, n_stage)}, device_id_type=MESH)
    loss_down = pltpu.make_async_remote_copy(
        src_ref=losst, dst_ref=losst, send_sem=ls_send, recv_sem=ls_recv,
        device_id={"stage": lax.rem(stage + last, n_stage)}, device_id_type=MESH)

    def transpose_weights(l, carry):
        for c in range(n_chunk):
            cols = slice(c * fc, (c + 1) * fc)
            w1t[l, cols, :] = w1s[l, :, cols].T
            w2t[l, :, cols] = w2s[l, cols, :].T
        return carry

    def fwd_layer(keep_grad, l, carry):
        @pl.when(stage == 0)
        def _():
            w1_copy(l).wait()
            w2_copy(l).wait()

        for step in range(1, n_data):
            gather_send(xs, l, xsend, xrecv, l, step).start()
        x_float, inv_rms, unit = unit_rows(xs[l, rep])
        normed = (unit * gain_ref[pl.ds(l, 1), :]).astype(BF)
        acc = x_float
        for c in range(n_chunk):
            cols = slice(c * fc, (c + 1) * fc)
            pre = dot(normed, w1s[l, :, cols])
            sq, th = gelu_tanh(pre)
            if keep_grad:
                gps[l, rep, :, cols] = gelu_grad(pre, sq, th)
            acc = acc + dot(gelu_val(pre, th), w2s[l, cols, :])
        xs[l + 1, rep] = acc.astype(BF)
        return carry

    @pl.when(stage == 0)
    def _():
        x_copy.wait()

    @pl.when(stage > 0)
    def _():
        def wait_and_transpose(l, carry):
            w1_copy(l).wait()
            w2_copy(l).wait()
            return transpose_weights(l, carry)

        lax.fori_loop(0, depth, wait_and_transpose, 0)
        chain_fwd.wait_recv()

    @pl.when(is_late)
    def _():
        lax.fori_loop(0, depth, functools.partial(fwd_layer, True), 0)

    @pl.when(jnp.logical_not(is_late))
    def _():
        lax.fori_loop(0, depth, functools.partial(fwd_layer, False), 0)

    @pl.when(stage < last)
    def _():
        chain_fwd.start()

    @pl.when(stage == last)
    def _():
        y_copy.wait()
        err = xs[depth, rep].astype(F32) - ybuf[...].astype(F32)
        dhs[depth, rep] = (err / tok_total).astype(BF)
        part = jnp.sum(err * err, axis=0, keepdims=True)
        tile = part[:, 0:128]
        for c in range(1, width // 128):
            tile = tile + part[:, c * 128:(c + 1) * 128]
        lossb[rep] = jnp.broadcast_to(tile, (8, 128))

    def ut_copy(l, who, slot):
        return pltpu.make_async_copy(utst.at[slot], ut_hbm.at[l, :, pl.ds(pl.multiple_of(who * rows, rows), rows)], ut_sem.at[slot])

    def rt_copy(l, who, slot):
        return pltpu.make_async_copy(rtst.at[slot], rt_hbm.at[l, :, pl.ds(pl.multiple_of(who * rows, rows), rows)], rt_sem.at[slot])

    def saved_block(b, carry):
        l = b // n_data
        step = lax.rem(b, n_data)
        who = peer(step)
        slot = lax.rem(b, 2)

        @pl.when(step > 0)
        def _():
            gather_recv(xs, l, xsend, xrecv, l, who).wait_recv()

        @pl.when(b >= 2)
        def _():
            ut_copy(l, who, slot).wait()
            rt_copy(l, who, slot).wait()

        _, _, unit = unit_rows(xs[l, who])
        normed = (unit * gain_ref[pl.ds(l, 1), :]).astype(BF)
        rtst[slot] = normed.T
        for c in range(n_chunk):
            cols = slice(c * fc, (c + 1) * fc)
            pre = dot(normed, w1s[l, :, cols])
            sq, th = gelu_tanh(pre)
            gps[l, who, :, cols] = gelu_grad(pre, sq, th)
            utst[slot, cols, :] = gelu_val(pre, th).T
        ut_copy(l, who, slot).start()
        rt_copy(l, who, slot).start()
        return carry

    def saved_all():
        lax.fori_loop(0, depth * n_data, saved_block, 0)
        for slot in range(2):
            ut_copy(0, 0, slot).wait()
            rt_copy(0, 0, slot).wait()

    @pl.when(stage == 0)
    def _():
        lax.fori_loop(0, depth, transpose_weights, 0)

    @pl.when(jnp.logical_not(is_late))
    def _():
        saved_all()

    def dao_copy(l):
        return pltpu.make_async_copy(dao.at[l], da_hbm.at[l, rep], dao_sem.at[l])

    def bwd_layer(i, carry):
        l = depth - 1 - i
        for step in range(1, n_data):
            gather_send(dhs, l + 1, dsend, drecv, l, step).start()
        d_out = dhs[l + 1, rep]
        _, inv_rms, unit = unit_rows(xs[l, rep])
        d_normed = None
        for c in range(n_chunk):
            cols = slice(c * fc, (c + 1) * fc)
            d_hidden = dot(d_out, w2t[l, :, cols])
            d_pre = (d_hidden * gps[l, rep, :, cols]).astype(BF)
            dao[l, :, cols] = d_pre
            part = dot(d_pre, w1t[l, cols, :])
            d_normed = part if d_normed is None else d_normed + part
        dao_copy(l).start()
        d_unit = d_normed * gain_ref[pl.ds(l, 1), :]
        d_x = inv_rms * (d_unit - unit * jnp.mean(d_unit * unit, axis=-1, keepdims=True))
        dhs[l, rep] = (d_out.astype(F32) + d_x).astype(BF)
        dgs[rep, pl.ds(l, 1), :] = jnp.sum(d_normed * unit, axis=0, keepdims=True)
        return carry

    @pl.when(stage < last)
    def _():
        chain_bwd.wait_recv()

    lax.fori_loop(0, depth, bwd_layer, 0)

    @pl.when(stage > 0)
    def _():
        chain_bwd.start()

    def dg_send(step):
        return pltpu.make_async_remote_copy(
            src_ref=dgs.at[rep], dst_ref=dgs.at[rep], send_sem=gsend.at[step - 1], recv_sem=grecv.at[rep],
            device_id={"data": peer(step)}, device_id_type=MESH)

    def dg_recv(who):
        return pltpu.make_async_remote_copy(
            src_ref=dgs.at[who], dst_ref=dgs.at[who], send_sem=gsend.at[0], recv_sem=grecv.at[who],
            device_id={"data": peer(1)}, device_id_type=MESH)

    def loss_send(step):
        return pltpu.make_async_remote_copy(
            src_ref=lossb.at[rep], dst_ref=lossb.at[rep], send_sem=lsend.at[step - 1], recv_sem=lrecv.at[rep],
            device_id={"data": peer(step)}, device_id_type=MESH)

    def loss_recv(who):
        return pltpu.make_async_remote_copy(
            src_ref=lossb.at[who], dst_ref=lossb.at[who], send_sem=lsend.at[0], recv_sem=lrecv.at[who],
            device_id={"data": peer(1)}, device_id_type=MESH)

    for step in range(1, n_data):
        dg_send(step).start()

    @pl.when(stage == last)
    def _():
        for step in range(1, n_data):
            loss_send(step).start()
        for step in range(1, n_data):
            loss_recv(peer(step)).wait_recv()
        total = lossb[0]
        for who in range(1, n_data):
            total = total + lossb[who]
        losst[...] = total
        for step in range(1, n_data):
            loss_send(step).wait_send()

    @pl.when(stage < last)
    def _():
        loss_down.wait_recv()

    @pl.when(stage > 0)
    def _():
        loss_down.start()

    @pl.when(is_late)
    def _():
        saved_all()

    def da_copy(l, who, slot):
        return pltpu.make_async_copy(dast.at[slot], da_hbm.at[l, who], da_sem.at[slot])

    def dh_copy(l):
        return pltpu.make_async_copy(dhs.at[l + 1], dh_hbm.at[l], dh_sem.at[l])

    def grad_block(b, carry):
        l = depth - 1 - b // (n_data - 1)
        step = 1 + lax.rem(b, n_data - 1)
        who = peer(step)
        slot = lax.rem(b, 2)
        gather_recv(dhs, l + 1, dsend, drecv, l, who).wait_recv()

        @pl.when(step == n_data - 1)
        def _():
            dh_copy(l).start()

        @pl.when(b >= 2)
        def _():
            da_copy(l, who, slot).wait()

        d_out = dhs[l + 1, who]
        for c in range(n_chunk):
            cols = slice(c * fc, (c + 1) * fc)
            d_hidden = dot(d_out, w2t[l, :, cols])
            dast[slot, :, cols] = (d_hidden * gps[l, who, :, cols]).astype(BF)
        da_copy(l, who, slot).start()
        return carry

    lax.fori_loop(0, depth * (n_data - 1), grad_block, 0)

    for step in range(1, n_data):
        dg_recv(peer(step)).wait_recv()
    dg_total = dgs[0]
    for who in range(1, n_data):
        dg_total = dg_total + dgs[who]
    dgain_ref[...] = dg_total
    loss_ref[...] = losst[...]

    for slot in range(2):
        da_copy(0, 0, slot).wait()
    for l in range(depth):
        dao_copy(l).wait()
        dh_copy(l).wait()
        for step in range(1, n_data):
            gather_send(xs, l, xsend, xrecv, l, step).wait_send()
            gather_send(dhs, l + 1, dsend, drecv, l, step).wait_send()
    for step in range(1, n_data):
        dg_send(step).wait_send()

    @pl.when(stage < last)
    def _():
        chain_fwd.wait_send()

    @pl.when(stage > 0)
    def _():
        chain_bwd.wait_send()
        loss_down.wait_send()


def weight_grad_kernel(count, rt_ref, ut_ref, da_ref, dh_ref, dg_ref, ls_ref, d_up_ref, d_down_ref, d_gain_ref, loss_ref):
    d_up_ref[0] = dot(rt_ref[0], da_ref[0])
    d_down_ref[0] = dot(ut_ref[0], dh_ref[0])
    d_gain_ref[...] = dg_ref[...]
    loss_ref[0] = jnp.sum(ls_ref[0:1, :]) / count


def solution(mesh):
    n_stage = mesh.shape["stage"]
    n_data = mesh.shape["data"]

    def local_step(x_in, y_tgt, w_up, w_down, gain):
        n_micro, tokens, width = x_in.shape
        rows = n_micro * tokens
        depth, _, ff = w_up.shape
        all_rows = n_data * rows
        fc = min(512, ff)
        any_spec = pl.BlockSpec(memory_space=pl.ANY)
        vmem_spec = pl.BlockSpec(memory_space=pltpu.VMEM)
        dma = pltpu.SemaphoreType.DMA
        r_t, u_t, d_pre, d_out, dg_all, loss_all = pl.pallas_call(
            functools.partial(chain_kernel, n_data, n_stage, float(all_rows), fc),
            out_shape=(
                jax.ShapeDtypeStruct((depth, width, all_rows), BF),
                jax.ShapeDtypeStruct((depth, ff, all_rows), BF),
                jax.ShapeDtypeStruct((depth, n_data, rows, ff), BF),
                jax.ShapeDtypeStruct((depth, n_data, rows, width), BF),
                jax.ShapeDtypeStruct((depth, width), F32),
                jax.ShapeDtypeStruct((8, 128), F32),
            ),
            in_specs=[any_spec, any_spec, any_spec, any_spec, vmem_spec],
            out_specs=(any_spec, any_spec, any_spec, any_spec, vmem_spec, vmem_spec),
            scratch_shapes=[
                pltpu.VMEM((depth, width, ff), BF),
                pltpu.VMEM((depth, ff, width), BF),
                pltpu.VMEM((depth, ff, width), BF),
                pltpu.VMEM((depth, width, ff), BF),
                pltpu.VMEM((depth + 1, n_data, rows, width), BF),
                pltpu.VMEM((depth + 1, n_data, rows, width), BF),
                pltpu.VMEM((depth, n_data, rows, ff), F32),
                pltpu.VMEM((depth, rows, ff), BF),
                pltpu.VMEM((2, rows, ff), BF),
                pltpu.VMEM((2, ff, rows), BF),
                pltpu.VMEM((2, width, rows), BF),
                pltpu.VMEM((rows, width), BF),
                pltpu.VMEM((n_data, depth, width), F32),
                pltpu.VMEM((n_data, 8, 128), F32),
                pltpu.VMEM((8, 128), F32),
                dma((depth,)), dma((depth,)), dma, dma,
                dma((depth, n_data - 1)), dma((depth, n_data)),
                dma((depth, n_data - 1)), dma((depth, n_data)),
                dma, dma, dma, dma,
                dma((n_data - 1,)), dma((n_data,)),
                dma((n_data - 1,)), dma((n_data,)),
                dma, dma,
                dma((2,)), dma((2,)), dma((2,)), dma((depth,)), dma((depth,)),
            ],
            compiler_params=pltpu.CompilerParams(
                collective_id=0, has_side_effects=True, vmem_limit_bytes=67043328),
            name="chain",
        )(x_in.reshape(rows, width), y_tgt.reshape(rows, width), w_up, w_down, gain)
        d_pre = d_pre.reshape(depth, all_rows, ff)
        d_out = d_out.reshape(depth, all_rows, width)
        return pl.pallas_call(
            functools.partial(weight_grad_kernel, float(all_rows * width)),
            grid=(depth, ff // fc),
            out_shape=(
                jax.ShapeDtypeStruct((depth, width, ff), F32),
                jax.ShapeDtypeStruct((depth, ff, width), F32),
                jax.ShapeDtypeStruct((depth, width), F32),
                jax.ShapeDtypeStruct((1,), F32),
            ),
            in_specs=[
                pl.BlockSpec((1, width, all_rows), lambda l, c: (l, 0, 0)),
                pl.BlockSpec((1, fc, all_rows), lambda l, c: (l, c, 0)),
                pl.BlockSpec((1, all_rows, fc), lambda l, c: (l, 0, c)),
                pl.BlockSpec((1, all_rows, width), lambda l, c: (l, 0, 0)),
                pl.BlockSpec((depth, width), lambda l, c: (0, 0)),
                pl.BlockSpec((8, 128), lambda l, c: (0, 0)),
            ],
            out_specs=(
                pl.BlockSpec((1, width, fc), lambda l, c: (l, 0, c)),
                pl.BlockSpec((1, fc, width), lambda l, c: (l, c, 0)),
                pl.BlockSpec((depth, width), lambda l, c: (0, 0)),
                pl.BlockSpec(memory_space=pltpu.SMEM),
            ),
            compiler_params=pltpu.CompilerParams(vmem_limit_bytes=48 << 20),
            name="weight_grads",
        )(r_t, u_t, d_pre, d_out, dg_all, loss_all)

    return jax.shard_map(local_step, mesh=mesh, in_specs=(P(("part", "data"), None, None), P(("part", "data"), None, None), P("stage", None, None), P("stage", None, None), P("stage", None)), out_specs=(P(("part", "stage"), None, None), P(("part", "stage"), None, None), P(("part", "stage"), None), P("part")), check_vma=False)
```

```python
import functools

import jax
import jax.numpy as jnp
from jax import lax
from jax.experimental import pallas as pl
from jax.experimental.pallas import tpu as pltpu
from jax.sharding import PartitionSpec as P

EPS = 1e-6
C1 = 0.7978845608028654
C2 = C1 * 0.044715
MESH = pl.DeviceIdType.MESH
BF = jnp.bfloat16
F32 = jnp.float32


def dot(lhs, rhs):
    return jnp.dot(lhs, rhs, preferred_element_type=F32)


def gelu_tanh(pre):
    sq = pre * pre
    return sq, jnp.tanh(pre * (C1 + C2 * sq))


def gelu_val(pre, th):
    half = 0.5 * pre
    return (half + half * th).astype(BF)


def gelu_grad(pre, sq, th):
    return (0.5 + 0.5 * th) + (0.5 * pre) * (1.0 - th * th) * (C1 + (3.0 * C2) * sq)


def unit_rows(rows):
    x_float = rows.astype(F32)
    inv_rms = lax.rsqrt(jnp.mean(x_float * x_float, axis=-1, keepdims=True) + EPS)
    return x_float, inv_rms, x_float * inv_rms


def chain_kernel(
    n_data, n_stage, tok_total, fc,
    x_hbm, y_hbm, w1_hbm, w2_hbm, gain_ref,
    w1s, w2s, rts, dhs, dgain_ref, loss_ref,
    w1t, w2t, xs, gps, dao, ybuf, dgs, lossb, losst,
    w1_sem, w2_sem, x_sem, y_sem, xsend, xrecv, dsend, drecv, cs_send, cs_recv, cd_send, cd_recv,
    gsend, grecv, lsend, lrecv, ls_send, ls_recv,
):
    rep = lax.axis_index("data")
    stage = lax.axis_index("stage")
    depth, width, ff = w1s.shape
    rows = xs.shape[2]
    last = n_stage - 1
    is_early = stage == 0
    is_late = stage >= n_stage - 2

    def peer(step):
        return lax.rem(rep + step, n_data)

    barrier = pltpu.get_barrier_semaphore()
    for step in range(1, n_data):
        pl.semaphore_signal(barrier, inc=1, device_id={"data": peer(step)}, device_id_type=MESH)
    pl.semaphore_signal(barrier, inc=1, device_id={"stage": lax.rem(stage + 1, n_stage)}, device_id_type=MESH)
    pl.semaphore_signal(barrier, inc=1, device_id={"stage": lax.rem(stage + last, n_stage)}, device_id_type=MESH)

    def w1_copy(l):
        return pltpu.make_async_copy(w1_hbm.at[l], w1s.at[l], w1_sem.at[l])

    def w2_copy(l):
        return pltpu.make_async_copy(w2_hbm.at[l], w2s.at[l], w2_sem.at[l])

    x_copy = pltpu.make_async_copy(x_hbm, xs.at[0, rep], x_sem)
    y_copy = pltpu.make_async_copy(y_hbm, ybuf, y_sem)

    @pl.when(stage == 0)
    def _():
        x_copy.start()

    w1_copy(0).start()
    w2_copy(0).start()

    @pl.when(stage > 0)
    def _():
        for l in range(1, depth):
            w1_copy(l).start()
            w2_copy(l).start()

    @pl.when(stage == last)
    def _():
        y_copy.start()

    def gather_send(buf, slot, send, recv, step):
        return pltpu.make_async_remote_copy(
            src_ref=buf.at[slot, rep], dst_ref=buf.at[slot, rep], send_sem=send.at[step - 1], recv_sem=recv.at[rep],
            device_id={"data": peer(step)}, device_id_type=MESH)

    def gather_recv(buf, slot, send, recv, who):
        return pltpu.make_async_remote_copy(
            src_ref=buf.at[slot, who], dst_ref=buf.at[slot, who], send_sem=send.at[0], recv_sem=recv.at[who],
            device_id={"data": peer(1)}, device_id_type=MESH)

    def x_gather_start():
        pl.semaphore_wait(barrier, n_data + 1)
        for step in range(1, n_data):
            gather_send(xs, 0, xsend, xrecv, step).start()

    chain_fwd = pltpu.make_async_remote_copy(
        src_ref=xs.at[depth, rep], dst_ref=xs.at[0, rep], send_sem=cs_send, recv_sem=cs_recv,
        device_id={"stage": lax.rem(stage + 1, n_stage)}, device_id_type=MESH)
    chain_bwd = pltpu.make_async_remote_copy(
        src_ref=dhs.at[0, rep], dst_ref=dhs.at[depth, rep], send_sem=cd_send, recv_sem=cd_recv,
        device_id={"stage": lax.rem(stage + last, n_stage)}, device_id_type=MESH)
    loss_down = pltpu.make_async_remote_copy(
        src_ref=losst, dst_ref=losst, send_sem=ls_send, recv_sem=ls_recv,
        device_id={"stage": lax.rem(stage + last, n_stage)}, device_id_type=MESH)

    def transpose_weights(l, carry):
        w1t[l] = w1s[l].T
        w2t[l] = w2s[l].T
        return carry

    def fwd_layers(loading, keep_grad):
        x_rows = xs[0, rep]
        for l in range(depth):
            x_float, _, unit = unit_rows(x_rows)
            normed = (unit * gain_ref[l:l + 1, :]).astype(BF)
            if loading:
                w1_copy(l).wait()
                if l < depth - 1:
                    w1_copy(l + 1).start()
            pre = dot(normed, w1s[l])
            sq, th = gelu_tanh(pre)
            if keep_grad:
                gps[l, rep] = gelu_grad(pre, sq, th)
            if loading:
                w2_copy(l).wait()
                if l < depth - 1:
                    w2_copy(l + 1).start()
            x_rows = (x_float + dot(gelu_val(pre, th), w2s[l])).astype(BF)
            xs[l + 1, rep] = x_rows

    @pl.when(stage == 0)
    def _():
        x_copy.wait()

    @pl.when(stage == 1)
    def _():
        for l in range(depth):
            w1_copy(l).wait()
            w2_copy(l).wait()

    @pl.when(stage > 1)
    def _():
        def wait_and_transpose(l, carry):
            w1_copy(l).wait()
            w2_copy(l).wait()
            return transpose_weights(l, carry)

        lax.fori_loop(0, depth, wait_and_transpose, 0)

    @pl.when(stage > 0)
    def _():
        chain_fwd.wait_recv()
        x_gather_start()

    @pl.when(is_early)
    def _():
        fwd_layers(True, False)

    @pl.when(is_late)
    def _():
        fwd_layers(False, True)

    @pl.when(jnp.logical_not(jnp.logical_or(is_early, is_late)))
    def _():
        fwd_layers(False, False)

    @pl.when(stage == 0)
    def _():
        x_gather_start()

    @pl.when(stage < last)
    def _():
        chain_fwd.start()

    @pl.when(stage == last)
    def _():
        y_copy.wait()
        err = xs[depth, rep].astype(F32) - ybuf[...].astype(F32)
        dhs[depth, rep] = (err / tok_total).astype(BF)
        part = jnp.sum(err * err, axis=0, keepdims=True)
        tile = part[:, 0:128]
        for c in range(1, width // 128):
            tile = tile + part[:, c * 128:(c + 1) * 128]
        lossb[rep] = jnp.broadcast_to(tile, (8, 128))

    def saved_layer(l, carry):
        x_float, _, unit = unit_rows(xs[l].reshape(n_data * rows, width))
        normed = (unit * gain_ref[pl.ds(l, 1), :]).astype(BF)
        rts[l] = normed.T
        acc = x_float
        for c in range(ff // fc):
            cols = slice(c * fc, (c + 1) * fc)
            pre = dot(normed, w1s[l, :, cols])
            sq, th = gelu_tanh(pre)
            gps[l, :, :, cols] = gelu_grad(pre, sq, th).reshape(n_data, rows, fc)
            hidden = gelu_val(pre, th)
            acc = acc + dot(hidden, w2s[l, cols, :])
            w2s[l, cols, :] = hidden.T

        @pl.when(l < depth - 1)
        def _():
            xs[l + 1] = acc.astype(BF).reshape(n_data, rows, width)

        return carry

    def saved_all():
        for step in range(1, n_data):
            gather_recv(xs, 0, xsend, xrecv, peer(step)).wait_recv()
        lax.fori_loop(0, depth, saved_layer, 0)

    @pl.when(stage < 2)
    def _():
        lax.fori_loop(0, depth, transpose_weights, 0)

    @pl.when(jnp.logical_not(is_late))
    def _():
        saved_all()

    def row_grad(d_out, d_normed, x_rows, l):
        _, inv_rms, unit = unit_rows(x_rows)
        d_unit = d_normed * gain_ref[pl.ds(l, 1), :]
        d_x = inv_rms * (d_unit - unit * jnp.mean(d_unit * unit, axis=-1, keepdims=True))
        return (d_out.astype(F32) + d_x).astype(BF), unit

    def bwd_layers():
        d_out = dhs[depth, rep]
        for l in reversed(range(depth)):
            d_pre = (dot(d_out, w2t[l]) * gps[l, rep]).astype(BF)
            dao[l] = d_pre
            d_normed = dot(d_pre, w1t[l])
            d_out, unit = row_grad(d_out, d_normed, xs[l, rep], l)
            dhs[l, rep] = d_out
            dgs[rep, l:l + 1, :] = jnp.sum(d_normed * unit, axis=0, keepdims=True)

    @pl.when(stage < last)
    def _():
        chain_bwd.wait_recv()

    for step in range(1, n_data):
        gather_send(dhs, depth, dsend, drecv, step).start()

    bwd_layers()

    @pl.when(stage > 0)
    def _():
        chain_bwd.start()

    def dg_send(step):
        return pltpu.make_async_remote_copy(
            src_ref=dgs.at[rep], dst_ref=dgs.at[rep], send_sem=gsend.at[step - 1], recv_sem=grecv.at[rep],
            device_id={"data": peer(step)}, device_id_type=MESH)

    def dg_recv(who):
        return pltpu.make_async_remote_copy(
            src_ref=dgs.at[who], dst_ref=dgs.at[who], send_sem=gsend.at[0], recv_sem=grecv.at[who],
            device_id={"data": peer(1)}, device_id_type=MESH)

    def loss_send(step):
        return pltpu.make_async_remote_copy(
            src_ref=lossb.at[rep], dst_ref=lossb.at[rep], send_sem=lsend.at[step - 1], recv_sem=lrecv.at[rep],
            device_id={"data": peer(step)}, device_id_type=MESH)

    def loss_recv(who):
        return pltpu.make_async_remote_copy(
            src_ref=lossb.at[who], dst_ref=lossb.at[who], send_sem=lsend.at[0], recv_sem=lrecv.at[who],
            device_id={"data": peer(1)}, device_id_type=MESH)

    for step in range(1, n_data):
        dg_send(step).start()

    @pl.when(stage == last)
    def _():
        for step in range(1, n_data):
            loss_send(step).start()
        for step in range(1, n_data):
            loss_recv(peer(step)).wait_recv()
        total = lossb[0]
        for who in range(1, n_data):
            total = total + lossb[who]
        losst[...] = total
        for step in range(1, n_data):
            loss_send(step).wait_send()

    @pl.when(stage < last)
    def _():
        loss_down.wait_recv()

    @pl.when(stage > 0)
    def _():
        loss_down.start()

    @pl.when(is_late)
    def _():
        saved_all()

    def own_rows(who):
        return pl.ds(pl.multiple_of(who * rows, rows), rows)

    def keep_block(l, carry):
        w1s[l, own_rows(rep), :] = dao[l]
        return carry

    lax.fori_loop(0, depth, keep_block, 0)

    def other_rows(who, l, down):
        d_out = dhs[l + 1, who]
        d_pre = (dot(d_out, w2t[l]) * gps[l, who]).astype(BF)
        w1s[l, own_rows(who), :] = d_pre
        if down:
            dhs[l, who], _ = row_grad(d_out, dot(d_pre, w1t[l]), xs[l, who], l)

    for step in (1, *range(n_data - 1, 1, -1)):
        who = peer(step)
        gather_recv(dhs, depth, dsend, drecv, who).wait_recv()

        def other_layer(i, carry):
            other_rows(who, depth - 1 - i, True)
            return carry

        lax.fori_loop(0, depth - 1, other_layer, 0)
        other_rows(who, 0, False)

    for step in range(1, n_data):
        dg_recv(peer(step)).wait_recv()
    dg_total = dgs[0]
    for who in range(1, n_data):
        dg_total = dg_total + dgs[who]
    dgain_ref[...] = dg_total
    loss_ref[...] = losst[...]

    for step in range(1, n_data):
        gather_send(xs, 0, xsend, xrecv, step).wait_send()
        gather_send(dhs, depth, dsend, drecv, step).wait_send()
        dg_send(step).wait_send()

    @pl.when(stage < last)
    def _():
        chain_fwd.wait_send()

    @pl.when(stage > 0)
    def _():
        chain_bwd.wait_send()
        loss_down.wait_send()


def weight_grad_kernel(count, slots, da_ref, ut_ref, rt_ref, dh_ref, dg_ref, ls_ref, d_up_hbm, d_down_hbm, d_gain_ref, loss_ref, up_st, down_st, up_sem, down_sem):
    depth, all_rows, ff = da_ref.shape
    fc = up_st.shape[2]
    n_chunk = ff // fc
    n_data, rows, width = dh_ref.shape[1:]

    def out_copies(k, slot):
        l = k // n_chunk
        cols = pl.ds(pl.multiple_of(lax.rem(k, n_chunk) * fc, fc), fc)
        return (pltpu.make_async_copy(up_st.at[slot], d_up_hbm.at[l, :, cols], up_sem.at[slot]),
                pltpu.make_async_copy(down_st.at[slot], d_down_hbm.at[l, cols, :], down_sem.at[slot]))

    def grads(k, carry):
        l = k // n_chunk
        cols = pl.ds(pl.multiple_of(lax.rem(k, n_chunk) * fc, fc), fc)
        slot = lax.rem(k, slots)

        @pl.when(k >= slots)
        def _():
            for copy in out_copies(k, slot):
                copy.wait()

        up_st[slot] = dot(rt_ref[l], da_ref[l, :, cols])
        down_st[slot] = dot(ut_ref[l, cols, :], dh_ref[l + 1].reshape(n_data * rows, width))
        for copy in out_copies(k, slot):
            copy.start()
        return carry

    lax.fori_loop(0, depth * n_chunk, grads, 0)
    d_gain_ref[...] = dg_ref[...]
    loss_ref[0] = jnp.sum(ls_ref[0:1, :]) / count
    for slot in range(slots):
        for copy in out_copies(0, slot):
            copy.wait()


def solution(mesh):
    n_stage = mesh.shape["stage"]
    n_data = mesh.shape["data"]

    def local_step(x_in, y_tgt, w_up, w_down, gain):
        n_micro, tokens, width = x_in.shape
        rows = n_micro * tokens
        depth, _, ff = w_up.shape
        all_rows = n_data * rows
        fc = ff // 2
        slots = 3
        any_spec = pl.BlockSpec(memory_space=pl.ANY)
        vmem_spec = pl.BlockSpec(memory_space=pltpu.VMEM)
        dma = pltpu.SemaphoreType.DMA
        saved = pl.pallas_call(
            functools.partial(chain_kernel, n_data, n_stage, float(all_rows), ff // 4),
            out_shape=(
                pltpu.VMEM((depth, width, ff), BF),
                pltpu.VMEM((depth, ff, width), BF),
                pltpu.VMEM((depth, width, all_rows), BF),
                pltpu.VMEM((depth + 1, n_data, rows, width), BF),
                pltpu.VMEM((depth, width), F32),
                pltpu.VMEM((8, 128), F32),
            ),
            in_specs=[any_spec, any_spec, any_spec, any_spec, vmem_spec],
            out_specs=(vmem_spec,) * 6,
            scratch_shapes=[
                pltpu.VMEM((depth, ff, width), BF),
                pltpu.VMEM((depth, width, ff), BF),
                pltpu.VMEM((depth + 1, n_data, rows, width), BF),
                pltpu.VMEM((depth, n_data, rows, ff), F32),
                pltpu.VMEM((depth, rows, ff), BF),
                pltpu.VMEM((rows, width), BF),
                pltpu.VMEM((n_data, depth, width), F32),
                pltpu.VMEM((n_data, 8, 128), F32),
                pltpu.VMEM((8, 128), F32),
                dma((depth,)), dma((depth,)), dma, dma,
                dma((n_data - 1,)), dma((n_data,)),
                dma((n_data - 1,)), dma((n_data,)),
                dma, dma, dma, dma,
                dma((n_data - 1,)), dma((n_data,)),
                dma((n_data - 1,)), dma((n_data,)),
                dma, dma,
            ],
            compiler_params=pltpu.CompilerParams(
                collective_id=0, has_side_effects=True, vmem_limit_bytes=43 << 20),
            name="chain",
        )(x_in.reshape(rows, width), y_tgt.reshape(rows, width), w_up, w_down, gain)
        return pl.pallas_call(
            functools.partial(weight_grad_kernel, float(all_rows * width), slots),
            out_shape=(
                jax.ShapeDtypeStruct((depth, width, ff), F32),
                jax.ShapeDtypeStruct((depth, ff, width), F32),
                jax.ShapeDtypeStruct((depth, width), F32),
                jax.ShapeDtypeStruct((1,), F32),
            ),
            in_specs=[vmem_spec] * 6,
            out_specs=(any_spec, any_spec, vmem_spec, pl.BlockSpec(memory_space=pltpu.SMEM)),
            scratch_shapes=[
                pltpu.VMEM((slots, width, fc), F32),
                pltpu.VMEM((slots, fc, width), F32),
                dma((slots,)), dma((slots,)),
            ],
            compiler_params=pltpu.CompilerParams(vmem_limit_bytes=20 << 20),
            name="weight_grads",
        )(*saved)

    return jax.shard_map(local_step, mesh=mesh, in_specs=(P(("part", "data"), None, None), P(("part", "data"), None, None), P("stage", None, None), P("stage", None, None), P("stage", None)), out_specs=(P(("part", "stage"), None, None), P(("part", "stage"), None, None), P(("part", "stage"), None), P("part")), check_vma=False)
```

```python
import functools

import jax
import jax.numpy as jnp
from jax import lax
from jax.experimental import pallas as pl
from jax.experimental.pallas import tpu as pltpu
from jax.sharding import PartitionSpec as P

EPS = 1e-6
C1 = 0.7978845608028654
C2 = C1 * 0.044715
MESH = pl.DeviceIdType.MESH
BF = jnp.bfloat16
F32 = jnp.float32


def dot(lhs, rhs):
    return jnp.dot(lhs, rhs, preferred_element_type=F32)


def gelu_tanh(pre):
    sq = pre * pre
    return sq, jnp.tanh(pre * (C1 + C2 * sq))


def gelu_val(pre, th):
    half = 0.5 * pre
    return (half + half * th).astype(BF)


def gelu_grad(pre, sq, th):
    return (0.5 + 0.5 * th) + (0.5 * pre) * (1.0 - th * th) * (C1 + (3.0 * C2) * sq)


def unit_rows(rows):
    x_float = rows.astype(F32)
    inv_rms = lax.rsqrt(jnp.mean(x_float * x_float, axis=-1, keepdims=True) + EPS)
    return x_float, inv_rms, x_float * inv_rms


def chain_kernel(
    n_data, n_stage, tok_total, fc,
    x_hbm, y_hbm, w1_hbm, w2_hbm, gain_ref,
    w1s, w2s, rts, dhs, dgain_ref, loss_ref,
    w1t, w2t, xs, gps, dao, ybuf, dgs, lossb, losst,
    w1_sem, w2_sem, x_sem, y_sem, xsend, xrecv, dsend, drecv, cs_send, cs_recv, cd_send, cd_recv,
    gsend, grecv, lsend, lrecv, ls_send, ls_recv,
):
    rep = lax.axis_index("data")
    stage = lax.axis_index("stage")
    depth, width, ff = w1s.shape
    rows = xs.shape[2]
    last = n_stage - 1
    is_first = stage == 0
    is_late = stage >= n_stage - 2

    def peer(step):
        return lax.rem(rep + step, n_data)

    barrier = pltpu.get_barrier_semaphore()
    for step in range(1, n_data):
        pl.semaphore_signal(barrier, inc=1, device_id={"data": peer(step)}, device_id_type=MESH)
    pl.semaphore_signal(barrier, inc=1, device_id={"stage": lax.rem(stage + 1, n_stage)}, device_id_type=MESH)
    pl.semaphore_signal(barrier, inc=1, device_id={"stage": lax.rem(stage + last, n_stage)}, device_id_type=MESH)

    def w1_copy(l):
        return pltpu.make_async_copy(w1_hbm.at[l], w1s.at[l], w1_sem.at[l])

    def w2_copy(l):
        return pltpu.make_async_copy(w2_hbm.at[l], w2s.at[l], w2_sem.at[l])

    x_copy = pltpu.make_async_copy(x_hbm, xs.at[0, rep], x_sem)
    y_copy = pltpu.make_async_copy(y_hbm, ybuf, y_sem)

    @pl.when(stage == 0)
    def _():
        x_copy.start()

    for l in range(2):
        w1_copy(l).start()
        w2_copy(l).start()

    @pl.when(stage > 0)
    def _():
        for l in range(2, depth):
            w1_copy(l).start()
            w2_copy(l).start()

    @pl.when(stage == last)
    def _():
        y_copy.start()

    def gather_send(buf, slot, send, recv, step):
        return pltpu.make_async_remote_copy(
            src_ref=buf.at[slot, rep], dst_ref=buf.at[slot, rep], send_sem=send.at[step - 1], recv_sem=recv.at[rep],
            device_id={"data": peer(step)}, device_id_type=MESH)

    def gather_recv(buf, slot, send, recv, who):
        return pltpu.make_async_remote_copy(
            src_ref=buf.at[slot, who], dst_ref=buf.at[slot, who], send_sem=send.at[0], recv_sem=recv.at[who],
            device_id={"data": peer(1)}, device_id_type=MESH)

    def x_gather_start():
        pl.semaphore_wait(barrier, n_data + 1)
        for step in range(1, n_data):
            gather_send(xs, 0, xsend, xrecv, step).start()

    chain_fwd = pltpu.make_async_remote_copy(
        src_ref=xs.at[depth, rep], dst_ref=xs.at[0, rep], send_sem=cs_send, recv_sem=cs_recv,
        device_id={"stage": lax.rem(stage + 1, n_stage)}, device_id_type=MESH)
    chain_bwd = pltpu.make_async_remote_copy(
        src_ref=dhs.at[0, rep], dst_ref=dhs.at[depth, rep], send_sem=cd_send, recv_sem=cd_recv,
        device_id={"stage": lax.rem(stage + last, n_stage)}, device_id_type=MESH)
    loss_down = pltpu.make_async_remote_copy(
        src_ref=losst, dst_ref=losst, send_sem=ls_send, recv_sem=ls_recv,
        device_id={"stage": lax.rem(stage + last, n_stage)}, device_id_type=MESH)

    def transpose_weights(l, carry):
        w1t[l] = w1s[l].T
        w2t[l] = w2s[l].T
        return carry

    def fwd_layers(loading, keep_grad):
        x_rows = xs[0, rep]
        for l in range(depth):
            x_float, _, unit = unit_rows(x_rows)
            normed = (unit * gain_ref[l:l + 1, :]).astype(BF)
            if loading:
                w1_copy(l).wait()
                if l < depth - 2:
                    w1_copy(l + 2).start()
            pre = dot(normed, w1s[l])
            sq, th = gelu_tanh(pre)
            if keep_grad:
                gps[l, rep] = gelu_grad(pre, sq, th)
            if loading:
                w2_copy(l).wait()
                if l < depth - 2:
                    w2_copy(l + 2).start()
            x_rows = (x_float + dot(gelu_val(pre, th), w2s[l])).astype(BF)
            xs[l + 1, rep] = x_rows

    @pl.when(stage == 0)
    def _():
        x_copy.wait()

    @pl.when(stage == 1)
    def _():
        for l in range(depth):
            w1_copy(l).wait()
            w2_copy(l).wait()

    @pl.when(stage > 1)
    def _():
        def wait_and_transpose(l, carry):
            w1_copy(l).wait()
            w2_copy(l).wait()
            return transpose_weights(l, carry)

        lax.fori_loop(0, depth, wait_and_transpose, 0)

    @pl.when(stage > 0)
    def _():
        chain_fwd.wait_recv()
        x_gather_start()

    @pl.when(is_first)
    def _():
        fwd_layers(True, False)

    @pl.when(is_late)
    def _():
        fwd_layers(False, True)

    @pl.when(jnp.logical_not(jnp.logical_or(is_first, is_late)))
    def _():
        fwd_layers(False, False)

    @pl.when(stage == 0)
    def _():
        x_gather_start()

    @pl.when(stage < last)
    def _():
        chain_fwd.start()

    @pl.when(stage == last)
    def _():
        y_copy.wait()
        err = xs[depth, rep].astype(F32) - ybuf[...].astype(F32)
        dhs[depth, rep] = (err / tok_total).astype(BF)
        part = jnp.sum(err * err, axis=0, keepdims=True)
        tile = part[:, 0:128]
        for c in range(1, width // 128):
            tile = tile + part[:, c * 128:(c + 1) * 128]
        lossb[rep] = jnp.broadcast_to(tile, (8, 128))

    def saved_layer(l, carry):
        x_float, _, unit = unit_rows(xs[l].reshape(n_data * rows, width))
        normed = (unit * gain_ref[pl.ds(l, 1), :]).astype(BF)
        rts[l] = normed.T
        acc = x_float
        for c in range(ff // fc):
            cols = slice(c * fc, (c + 1) * fc)
            pre = dot(normed, w1s[l, :, cols])
            sq, th = gelu_tanh(pre)
            gps[l, :, :, cols] = gelu_grad(pre, sq, th).reshape(n_data, rows, fc)
            hidden = gelu_val(pre, th)
            acc = acc + dot(hidden, w2s[l, cols, :])
            w2s[l, cols, :] = hidden.T

        @pl.when(l < depth - 1)
        def _():
            xs[l + 1] = acc.astype(BF).reshape(n_data, rows, width)

        return carry

    def saved_all():
        for step in range(1, n_data):
            gather_recv(xs, 0, xsend, xrecv, peer(step)).wait_recv()
        lax.fori_loop(0, depth, saved_layer, 0)

    @pl.when(stage < 2)
    def _():
        lax.fori_loop(0, depth, transpose_weights, 0)

    @pl.when(jnp.logical_not(is_late))
    def _():
        saved_all()

    def row_grad(d_out, d_normed, x_rows, l):
        _, inv_rms, unit = unit_rows(x_rows)
        d_unit = d_normed * gain_ref[pl.ds(l, 1), :]
        d_x = inv_rms * (d_unit - unit * jnp.mean(d_unit * unit, axis=-1, keepdims=True))
        return (d_out.astype(F32) + d_x).astype(BF), unit

    def bwd_layers():
        d_out = dhs[depth, rep]
        for l in reversed(range(depth)):
            d_pre = (dot(d_out, w2t[l]) * gps[l, rep]).astype(BF)
            dao[l] = d_pre
            d_normed = dot(d_pre, w1t[l])
            d_out, unit = row_grad(d_out, d_normed, xs[l, rep], l)
            dhs[l, rep] = d_out
            dgs[rep, l:l + 1, :] = jnp.sum(d_normed * unit, axis=0, keepdims=True)

    @pl.when(stage < last)
    def _():
        chain_bwd.wait_recv()

    for step in range(1, n_data):
        gather_send(dhs, depth, dsend, drecv, step).start()

    bwd_layers()

    @pl.when(stage > 0)
    def _():
        chain_bwd.start()

    def dg_send(step):
        return pltpu.make_async_remote_copy(
            src_ref=dgs.at[rep], dst_ref=dgs.at[rep], send_sem=gsend.at[step - 1], recv_sem=grecv.at[rep],
            device_id={"data": peer(step)}, device_id_type=MESH)

    def dg_recv(who):
        return pltpu.make_async_remote_copy(
            src_ref=dgs.at[who], dst_ref=dgs.at[who], send_sem=gsend.at[0], recv_sem=grecv.at[who],
            device_id={"data": peer(1)}, device_id_type=MESH)

    def loss_send(step):
        return pltpu.make_async_remote_copy(
            src_ref=lossb.at[rep], dst_ref=lossb.at[rep], send_sem=lsend.at[step - 1], recv_sem=lrecv.at[rep],
            device_id={"data": peer(step)}, device_id_type=MESH)

    def loss_recv(who):
        return pltpu.make_async_remote_copy(
            src_ref=lossb.at[who], dst_ref=lossb.at[who], send_sem=lsend.at[0], recv_sem=lrecv.at[who],
            device_id={"data": peer(1)}, device_id_type=MESH)

    for step in range(1, n_data):
        dg_send(step).start()

    @pl.when(stage == last)
    def _():
        for step in range(1, n_data):
            loss_send(step).start()
        for step in range(1, n_data):
            loss_recv(peer(step)).wait_recv()
        total = lossb[0]
        for who in range(1, n_data):
            total = total + lossb[who]
        losst[...] = total
        for step in range(1, n_data):
            loss_send(step).wait_send()

    @pl.when(stage < last)
    def _():
        loss_down.wait_recv()

    @pl.when(stage > 0)
    def _():
        loss_down.start()

    @pl.when(is_late)
    def _():
        saved_all()

    def own_rows(who):
        return pl.ds(pl.multiple_of(who * rows, rows), rows)

    def other_layers(whos, keep_own):
        for who in whos:
            gather_recv(dhs, depth, dsend, drecv, who).wait_recv()
        d_out = [dhs[depth, who] for who in whos]
        for l in reversed(range(depth)):
            if keep_own:
                w1s[l, own_rows(rep), :] = dao[l]
            for i, who in enumerate(whos):
                d_pre = (dot(d_out[i], w2t[l]) * gps[l, who]).astype(BF)
                w1s[l, own_rows(who), :] = d_pre
                if l > 0:
                    d_out[i], _ = row_grad(d_out[i], dot(d_pre, w1t[l]), xs[l, who], l)
                    dhs[l, who] = d_out[i]

    other_layers([peer(1)], True)
    other_layers([peer(step) for step in range(n_data - 1, 1, -1)], False)

    for step in range(1, n_data):
        dg_recv(peer(step)).wait_recv()
    dg_total = dgs[0]
    for who in range(1, n_data):
        dg_total = dg_total + dgs[who]
    dgain_ref[...] = dg_total
    loss_ref[...] = losst[...]

    for step in range(1, n_data):
        gather_send(xs, 0, xsend, xrecv, step).wait_send()
        gather_send(dhs, depth, dsend, drecv, step).wait_send()
        dg_send(step).wait_send()

    @pl.when(stage < last)
    def _():
        chain_fwd.wait_send()

    @pl.when(stage > 0)
    def _():
        chain_bwd.wait_send()
        loss_down.wait_send()


def weight_grad_kernel(count, slots, da_ref, ut_ref, rt_ref, dh_ref, dg_ref, ls_ref, d_up_hbm, d_down_hbm, d_gain_ref, loss_ref, up_st, down_st, up_sem, down_sem):
    depth, all_rows, ff = da_ref.shape
    fc = up_st.shape[2]
    n_chunk = ff // fc
    n_data, rows, width = dh_ref.shape[1:]

    def out_copies(k, slot):
        l = k // n_chunk
        cols = pl.ds(pl.multiple_of(lax.rem(k, n_chunk) * fc, fc), fc)
        return (pltpu.make_async_copy(up_st.at[slot], d_up_hbm.at[l, :, cols], up_sem.at[slot]),
                pltpu.make_async_copy(down_st.at[slot], d_down_hbm.at[l, cols, :], down_sem.at[slot]))

    def grads(k, carry):
        l = k // n_chunk
        cols = pl.ds(pl.multiple_of(lax.rem(k, n_chunk) * fc, fc), fc)
        slot = lax.rem(k, slots)

        @pl.when(k >= slots)
        def _():
            for copy in out_copies(k, slot):
                copy.wait()

        up_st[slot] = dot(rt_ref[l], da_ref[l, :, cols])
        down_st[slot] = dot(ut_ref[l, cols, :], dh_ref[l + 1].reshape(n_data * rows, width))
        for copy in out_copies(k, slot):
            copy.start()
        return carry

    lax.fori_loop(0, depth * n_chunk, grads, 0)
    d_gain_ref[...] = dg_ref[...]
    loss_ref[0] = jnp.sum(ls_ref[0:1, :]) / count
    for slot in range(slots):
        for copy in out_copies(0, slot):
            copy.wait()


def solution(mesh):
    n_stage = mesh.shape["stage"]
    n_data = mesh.shape["data"]

    def local_step(x_in, y_tgt, w_up, w_down, gain):
        n_micro, tokens, width = x_in.shape
        rows = n_micro * tokens
        depth, _, ff = w_up.shape
        all_rows = n_data * rows
        fc = ff // 2
        slots = 3
        any_spec = pl.BlockSpec(memory_space=pl.ANY)
        vmem_spec = pl.BlockSpec(memory_space=pltpu.VMEM)
        dma = pltpu.SemaphoreType.DMA
        saved = pl.pallas_call(
            functools.partial(chain_kernel, n_data, n_stage, float(all_rows), ff // 4),
            out_shape=(
                pltpu.VMEM((depth, width, ff), BF),
                pltpu.VMEM((depth, ff, width), BF),
                pltpu.VMEM((depth, width, all_rows), BF),
                pltpu.VMEM((depth + 1, n_data, rows, width), BF),
                pltpu.VMEM((depth, width), F32),
                pltpu.VMEM((8, 128), F32),
            ),
            in_specs=[any_spec, any_spec, any_spec, any_spec, vmem_spec],
            out_specs=(vmem_spec,) * 6,
            scratch_shapes=[
                pltpu.VMEM((depth, ff, width), BF),
                pltpu.VMEM((depth, width, ff), BF),
                pltpu.VMEM((depth + 1, n_data, rows, width), BF),
                pltpu.VMEM((depth, n_data, rows, ff), F32),
                pltpu.VMEM((depth, rows, ff), BF),
                pltpu.VMEM((rows, width), BF),
                pltpu.VMEM((n_data, depth, width), F32),
                pltpu.VMEM((n_data, 8, 128), F32),
                pltpu.VMEM((8, 128), F32),
                dma((depth,)), dma((depth,)), dma, dma,
                dma((n_data - 1,)), dma((n_data,)),
                dma((n_data - 1,)), dma((n_data,)),
                dma, dma, dma, dma,
                dma((n_data - 1,)), dma((n_data,)),
                dma((n_data - 1,)), dma((n_data,)),
                dma, dma,
            ],
            compiler_params=pltpu.CompilerParams(
                collective_id=0, has_side_effects=True, vmem_limit_bytes=43 << 20),
            name="chain",
        )(x_in.reshape(rows, width), y_tgt.reshape(rows, width), w_up, w_down, gain)
        return pl.pallas_call(
            functools.partial(weight_grad_kernel, float(all_rows * width), slots),
            out_shape=(
                jax.ShapeDtypeStruct((depth, width, ff), F32),
                jax.ShapeDtypeStruct((depth, ff, width), F32),
                jax.ShapeDtypeStruct((depth, width), F32),
                jax.ShapeDtypeStruct((1,), F32),
            ),
            in_specs=[vmem_spec] * 6,
            out_specs=(any_spec, any_spec, vmem_spec, pl.BlockSpec(memory_space=pltpu.SMEM)),
            scratch_shapes=[
                pltpu.VMEM((slots, width, fc), F32),
                pltpu.VMEM((slots, fc, width), F32),
                dma((slots,)), dma((slots,)),
            ],
            compiler_params=pltpu.CompilerParams(vmem_limit_bytes=20 << 20),
            name="weight_grads",
        )(*saved)

    return jax.shard_map(local_step, mesh=mesh, in_specs=(P(("part", "data"), None, None), P(("part", "data"), None, None), P("stage", None, None), P("stage", None, None), P("stage", None)), out_specs=(P(("part", "stage"), None, None), P(("part", "stage"), None, None), P(("part", "stage"), None), P("part")), check_vma=False)
```

```python
import functools

import jax
import jax.numpy as jnp
from jax import lax
from jax.experimental import pallas as pl
from jax.experimental.pallas import tpu as pltpu
from jax.sharding import PartitionSpec as P

EPS = 1e-6
C1 = 0.7978845608028654
C2 = C1 * 0.044715
MESH = pl.DeviceIdType.MESH
BF = jnp.bfloat16
F32 = jnp.float32


def dot(lhs, rhs):
    return jnp.dot(lhs, rhs, preferred_element_type=F32)


def gelu_tanh(pre):
    sq = pre * pre
    return sq, jnp.tanh(pre * (C1 + C2 * sq))


def gelu_val(pre, th):
    half = 0.5 * pre
    return (half + half * th).astype(BF)


def gelu_grad(pre, sq, th):
    return (0.5 + 0.5 * th) + (0.5 * pre) * (1.0 - th * th) * (C1 + (3.0 * C2) * sq)


def unit_rows(rows):
    x_float = rows.astype(F32)
    inv_rms = lax.rsqrt(jnp.mean(x_float * x_float, axis=-1, keepdims=True) + EPS)
    return x_float, inv_rms, x_float * inv_rms


def chain_kernel(
    n_data, n_stage, tok_total, fc,
    x_hbm, y_hbm, w1_hbm, w2_hbm, gain_ref,
    w1s, w2s, rts, dhs, dgain_ref, loss_ref,
    w1t, w2t, xs, gps, dao, ybuf, dgs, lossb, losst,
    w1_sem, w2_sem, x_sem, y_sem, xsend, xrecv, dsend, drecv, cs_send, cs_recv, cd_send, cd_recv,
    gsend, grecv, lsend, lrecv, ls_send, ls_recv,
):
    rep = lax.axis_index("data")
    stage = lax.axis_index("stage")
    depth, width, ff = w1s.shape
    rows = xs.shape[2]
    last = n_stage - 1
    is_first = stage == 0
    is_late = stage >= n_stage - 2

    def peer(step):
        return lax.rem(rep + step, n_data)

    barrier = pltpu.get_barrier_semaphore()
    for step in range(1, n_data):
        pl.semaphore_signal(barrier, inc=1, device_id={"data": peer(step)}, device_id_type=MESH)
    pl.semaphore_signal(barrier, inc=1, device_id={"stage": lax.rem(stage + 1, n_stage)}, device_id_type=MESH)
    pl.semaphore_signal(barrier, inc=1, device_id={"stage": lax.rem(stage + last, n_stage)}, device_id_type=MESH)

    def w1_copy(l):
        return pltpu.make_async_copy(w1_hbm.at[l], w1s.at[l], w1_sem.at[l])

    def w2_copy(l):
        return pltpu.make_async_copy(w2_hbm.at[l], w2s.at[l], w2_sem.at[l])

    x_copy = pltpu.make_async_copy(x_hbm, xs.at[0, rep], x_sem)
    y_copy = pltpu.make_async_copy(y_hbm, ybuf, y_sem)

    @pl.when(stage == 0)
    def _():
        x_copy.start()

    for l in range(2):
        w1_copy(l).start()
        w2_copy(l).start()

    @pl.when(stage > 0)
    def _():
        for l in range(2, depth):
            w1_copy(l).start()
            w2_copy(l).start()

    @pl.when(stage == last)
    def _():
        y_copy.start()

    def gather_send(buf, slot, send, recv, step):
        return pltpu.make_async_remote_copy(
            src_ref=buf.at[slot, rep], dst_ref=buf.at[slot, rep], send_sem=send.at[step - 1], recv_sem=recv.at[rep],
            device_id={"data": peer(step)}, device_id_type=MESH)

    def gather_recv(buf, slot, send, recv, who):
        return pltpu.make_async_remote_copy(
            src_ref=buf.at[slot, who], dst_ref=buf.at[slot, who], send_sem=send.at[0], recv_sem=recv.at[who],
            device_id={"data": peer(1)}, device_id_type=MESH)

    def x_gather_start():
        pl.semaphore_wait(barrier, n_data + 1)
        for step in range(1, n_data):
            gather_send(xs, 0, xsend, xrecv, step).start()

    chain_fwd = pltpu.make_async_remote_copy(
        src_ref=xs.at[depth, rep], dst_ref=xs.at[0, rep], send_sem=cs_send, recv_sem=cs_recv,
        device_id={"stage": lax.rem(stage + 1, n_stage)}, device_id_type=MESH)
    chain_bwd = pltpu.make_async_remote_copy(
        src_ref=dhs.at[0, rep], dst_ref=dhs.at[depth, rep], send_sem=cd_send, recv_sem=cd_recv,
        device_id={"stage": lax.rem(stage + last, n_stage)}, device_id_type=MESH)
    loss_down = pltpu.make_async_remote_copy(
        src_ref=losst, dst_ref=losst, send_sem=ls_send, recv_sem=ls_recv,
        device_id={"stage": lax.rem(stage + last, n_stage)}, device_id_type=MESH)

    def transpose_weights(l, carry):
        w1t[l] = w1s[l].T
        w2t[l] = w2s[l].T
        return carry

    def fwd_layer(loading, keep_grad, l, x_rows):
        def arrive(copy):
            copy(l).wait()

            @pl.when(l < depth - 2)
            def _():
                copy(l + 2).start()

        x_float, _, unit = unit_rows(x_rows)
        normed = (unit * gain_ref[pl.ds(l, 1), :]).astype(BF)
        if loading:
            arrive(w1_copy)
        pre = dot(normed, w1s[l])
        sq, th = gelu_tanh(pre)
        if keep_grad:
            gps[l, rep] = gelu_grad(pre, sq, th)
        if loading:
            arrive(w2_copy)
        x_rows = (x_float + dot(gelu_val(pre, th), w2s[l])).astype(BF)
        xs[l + 1, rep] = x_rows
        return x_rows

    def fwd_layers(loading, keep_grad):
        if loading:
            lax.fori_loop(0, depth, functools.partial(fwd_layer, True, keep_grad), xs[0, rep])
            return
        x_rows = xs[0, rep]
        for l in range(depth):
            x_rows = fwd_layer(False, keep_grad, l, x_rows)

    @pl.when(stage == 0)
    def _():
        x_copy.wait()

    @pl.when(stage == 1)
    def _():
        for l in range(depth):
            w1_copy(l).wait()
            w2_copy(l).wait()

    @pl.when(stage > 1)
    def _():
        def wait_and_transpose(l, carry):
            w1_copy(l).wait()
            w2_copy(l).wait()
            return transpose_weights(l, carry)

        lax.fori_loop(0, depth, wait_and_transpose, 0)

    @pl.when(stage > 0)
    def _():
        chain_fwd.wait_recv()
        x_gather_start()

    @pl.when(is_first)
    def _():
        fwd_layers(True, False)

    @pl.when(is_late)
    def _():
        fwd_layers(False, True)

    @pl.when(jnp.logical_not(jnp.logical_or(is_first, is_late)))
    def _():
        fwd_layers(False, False)

    @pl.when(stage == 0)
    def _():
        x_gather_start()

    @pl.when(stage < last)
    def _():
        chain_fwd.start()

    @pl.when(stage == last)
    def _():
        y_copy.wait()
        err = xs[depth, rep].astype(F32) - ybuf[...].astype(F32)
        dhs[depth, rep] = (err / tok_total).astype(BF)
        part = jnp.sum(err * err, axis=0, keepdims=True)
        tile = part[:, 0:128]
        for c in range(1, width // 128):
            tile = tile + part[:, c * 128:(c + 1) * 128]
        lossb[rep] = jnp.broadcast_to(tile, (8, 128))

    def saved_layer(l, carry):
        x_float, _, unit = unit_rows(xs[l].reshape(n_data * rows, width))
        normed = (unit * gain_ref[pl.ds(l, 1), :]).astype(BF)
        rts[l] = normed.T
        acc = x_float
        for c in range(ff // fc):
            cols = slice(c * fc, (c + 1) * fc)
            pre = dot(normed, w1s[l, :, cols])
            sq, th = gelu_tanh(pre)
            gps[l, :, :, cols] = gelu_grad(pre, sq, th).reshape(n_data, rows, fc)
            hidden = gelu_val(pre, th)
            acc = acc + dot(hidden, w2s[l, cols, :])
            w2s[l, cols, :] = hidden.T

        @pl.when(l < depth - 1)
        def _():
            xs[l + 1] = acc.astype(BF).reshape(n_data, rows, width)

        return carry

    def saved_all():
        for step in range(1, n_data):
            gather_recv(xs, 0, xsend, xrecv, peer(step)).wait_recv()
        lax.fori_loop(0, depth, saved_layer, 0)

    @pl.when(stage < 2)
    def _():
        lax.fori_loop(0, depth, transpose_weights, 0)

    @pl.when(jnp.logical_not(is_late))
    def _():
        saved_all()

    def row_grad(d_out, d_normed, x_rows, l):
        _, inv_rms, unit = unit_rows(x_rows)
        d_unit = d_normed * gain_ref[pl.ds(l, 1), :]
        d_x = inv_rms * (d_unit - unit * jnp.mean(d_unit * unit, axis=-1, keepdims=True))
        return (d_out.astype(F32) + d_x).astype(BF), unit

    def bwd_layers():
        d_out = dhs[depth, rep]
        for l in reversed(range(depth)):
            d_pre = (dot(d_out, w2t[l]) * gps[l, rep]).astype(BF)
            dao[l] = d_pre
            d_normed = dot(d_pre, w1t[l])
            d_out, unit = row_grad(d_out, d_normed, xs[l, rep], l)
            dhs[l, rep] = d_out
            dgs[rep, l:l + 1, :] = jnp.sum(d_normed * unit, axis=0, keepdims=True)

    @pl.when(stage < last)
    def _():
        chain_bwd.wait_recv()

    for step in range(1, n_data):
        gather_send(dhs, depth, dsend, drecv, step).start()

    bwd_layers()

    @pl.when(stage > 0)
    def _():
        chain_bwd.start()

    def dg_send(step):
        return pltpu.make_async_remote_copy(
            src_ref=dgs.at[rep], dst_ref=dgs.at[rep], send_sem=gsend.at[step - 1], recv_sem=grecv.at[rep],
            device_id={"data": peer(step)}, device_id_type=MESH)

    def dg_recv(who):
        return pltpu.make_async_remote_copy(
            src_ref=dgs.at[who], dst_ref=dgs.at[who], send_sem=gsend.at[0], recv_sem=grecv.at[who],
            device_id={"data": peer(1)}, device_id_type=MESH)

    def loss_send(step):
        return pltpu.make_async_remote_copy(
            src_ref=lossb.at[rep], dst_ref=lossb.at[rep], send_sem=lsend.at[step - 1], recv_sem=lrecv.at[rep],
            device_id={"data": peer(step)}, device_id_type=MESH)

    def loss_recv(who):
        return pltpu.make_async_remote_copy(
            src_ref=lossb.at[who], dst_ref=lossb.at[who], send_sem=lsend.at[0], recv_sem=lrecv.at[who],
            device_id={"data": peer(1)}, device_id_type=MESH)

    for step in range(1, n_data):
        dg_send(step).start()

    @pl.when(stage == last)
    def _():
        for step in range(1, n_data):
            loss_send(step).start()
        for step in range(1, n_data):
            loss_recv(peer(step)).wait_recv()
        total = lossb[0]
        for who in range(1, n_data):
            total = total + lossb[who]
        losst[...] = total
        for step in range(1, n_data):
            loss_send(step).wait_send()

    @pl.when(stage < last)
    def _():
        loss_down.wait_recv()

    @pl.when(stage > 0)
    def _():
        loss_down.start()

    @pl.when(is_late)
    def _():
        saved_all()

    def own_rows(who):
        return pl.ds(pl.multiple_of(who * rows, rows), rows)

    def other_layers(whos, keep_own):
        for who in whos:
            gather_recv(dhs, depth, dsend, drecv, who).wait_recv()
        d_out = [dhs[depth, who] for who in whos]
        for l in reversed(range(depth)):
            if keep_own:
                w1s[l, own_rows(rep), :] = dao[l]
            for i, who in enumerate(whos):
                d_pre = (dot(d_out[i], w2t[l]) * gps[l, who]).astype(BF)
                w1s[l, own_rows(who), :] = d_pre
                if l > 0:
                    d_out[i], _ = row_grad(d_out[i], dot(d_pre, w1t[l]), xs[l, who], l)
                    dhs[l, who] = d_out[i]

    other_layers([peer(1)], True)
    other_layers([peer(step) for step in range(n_data - 1, 1, -1)], False)

    for step in range(1, n_data):
        dg_recv(peer(step)).wait_recv()
    dg_total = dgs[0]
    for who in range(1, n_data):
        dg_total = dg_total + dgs[who]
    dgain_ref[...] = dg_total
    loss_ref[...] = losst[...]

    for step in range(1, n_data):
        gather_send(xs, 0, xsend, xrecv, step).wait_send()
        gather_send(dhs, depth, dsend, drecv, step).wait_send()
        dg_send(step).wait_send()

    @pl.when(stage < last)
    def _():
        chain_fwd.wait_send()

    @pl.when(stage > 0)
    def _():
        chain_bwd.wait_send()
        loss_down.wait_send()


def weight_grad_kernel(count, slots, da_ref, ut_ref, rt_ref, dh_ref, dg_ref, ls_ref, d_up_hbm, d_down_hbm, d_gain_ref, loss_ref, up_st, down_st, up_sem, down_sem):
    depth, all_rows, ff = da_ref.shape
    n_data, rows, width = dh_ref.shape[1:]
    half, quarter = ff // 2, ff // 4
    pieces = []
    for l in range(depth):
        sizes = (half, half)
        if l == 0:
            sizes = (quarter, quarter, half)
        elif l == depth - 1:
            sizes = (half, quarter, quarter)
        for i, size in enumerate(sizes):
            pieces.append((l, sum(sizes[:i]), size))

    pending = [()] * slots
    for k, (l, first, size) in enumerate(pieces):
        cols = pl.ds(first, size)
        slot = k % slots
        for copy in pending[slot]:
            copy.wait()
        up_st[slot, :, :size] = dot(rt_ref[l], da_ref[l, :, cols])
        down_st[slot, :size, :] = dot(ut_ref[l, cols, :], dh_ref[l + 1].reshape(n_data * rows, width))
        pending[slot] = (
            pltpu.make_async_copy(up_st.at[slot, :, pl.ds(0, size)], d_up_hbm.at[l, :, cols], up_sem.at[slot]),
            pltpu.make_async_copy(down_st.at[slot, pl.ds(0, size), :], d_down_hbm.at[l, cols, :], down_sem.at[slot]))
        for copy in pending[slot]:
            copy.start()
    d_gain_ref[...] = dg_ref[...]
    loss_ref[0] = jnp.sum(ls_ref[0:1, :]) / count
    for copies in pending:
        for copy in copies:
            copy.wait()


def solution(mesh):
    n_stage = mesh.shape["stage"]
    n_data = mesh.shape["data"]

    def local_step(x_in, y_tgt, w_up, w_down, gain):
        n_micro, tokens, width = x_in.shape
        rows = n_micro * tokens
        depth, _, ff = w_up.shape
        all_rows = n_data * rows
        fc = ff // 2
        slots = 3
        any_spec = pl.BlockSpec(memory_space=pl.ANY)
        vmem_spec = pl.BlockSpec(memory_space=pltpu.VMEM)
        dma = pltpu.SemaphoreType.DMA
        saved = pl.pallas_call(
            functools.partial(chain_kernel, n_data, n_stage, float(all_rows), ff // 4),
            out_shape=(
                pltpu.VMEM((depth, width, ff), BF),
                pltpu.VMEM((depth, ff, width), BF),
                pltpu.VMEM((depth, width, all_rows), BF),
                pltpu.VMEM((depth + 1, n_data, rows, width), BF),
                pltpu.VMEM((depth, width), F32),
                pltpu.VMEM((8, 128), F32),
            ),
            in_specs=[any_spec, any_spec, any_spec, any_spec, vmem_spec],
            out_specs=(vmem_spec,) * 6,
            scratch_shapes=[
                pltpu.VMEM((depth, ff, width), BF),
                pltpu.VMEM((depth, width, ff), BF),
                pltpu.VMEM((depth + 1, n_data, rows, width), BF),
                pltpu.VMEM((depth, n_data, rows, ff), F32),
                pltpu.VMEM((depth, rows, ff), BF),
                pltpu.VMEM((rows, width), BF),
                pltpu.VMEM((n_data, depth, width), F32),
                pltpu.VMEM((n_data, 8, 128), F32),
                pltpu.VMEM((8, 128), F32),
                dma((depth,)), dma((depth,)), dma, dma,
                dma((n_data - 1,)), dma((n_data,)),
                dma((n_data - 1,)), dma((n_data,)),
                dma, dma, dma, dma,
                dma((n_data - 1,)), dma((n_data,)),
                dma((n_data - 1,)), dma((n_data,)),
                dma, dma,
            ],
            compiler_params=pltpu.CompilerParams(
                collective_id=0, has_side_effects=True, vmem_limit_bytes=43 << 20),
            name="chain",
        )(x_in.reshape(rows, width), y_tgt.reshape(rows, width), w_up, w_down, gain)
        return pl.pallas_call(
            functools.partial(weight_grad_kernel, float(all_rows * width), slots),
            out_shape=(
                jax.ShapeDtypeStruct((depth, width, ff), F32),
                jax.ShapeDtypeStruct((depth, ff, width), F32),
                jax.ShapeDtypeStruct((depth, width), F32),
                jax.ShapeDtypeStruct((1,), F32),
            ),
            in_specs=[vmem_spec] * 6,
            out_specs=(any_spec, any_spec, vmem_spec, pl.BlockSpec(memory_space=pltpu.SMEM)),
            scratch_shapes=[
                pltpu.VMEM((slots, width, fc), F32),
                pltpu.VMEM((slots, fc, width), F32),
                dma((slots,)), dma((slots,)),
            ],
            compiler_params=pltpu.CompilerParams(vmem_limit_bytes=20 << 20),
            name="weight_grads",
        )(*saved)

    return jax.shard_map(local_step, mesh=mesh, in_specs=(P(("part", "data"), None, None), P(("part", "data"), None, None), P("stage", None, None), P("stage", None, None), P("stage", None)), out_specs=(P(("part", "stage"), None, None), P(("part", "stage"), None, None), P(("part", "stage"), None), P("part")), check_vma=False)
```
